1024 devices in a mesh: tensor: 4 (over y), expert: 64 (over z, core), dp: 4 (over x).
Axes of the slice: x: 4, y: 4, z: 32, core: 2. Of those that a mesh axis runs over, the one named last changes fastest.
Arguments:
- grad_out: bfloat16 [16384, 4096], P(('expert', 'dp')), may hold values from -6 to 6
- route_ids: int32 [16384, 8], P(('expert', 'dp')), may hold values from 0 to 127, all different within a row; in each aligned block of 64 rows (0 to 63, 64 to 127, ...) at most 6 rows name the same one
- route_probs: bfloat16 [16384, 8], P(('expert', 'dp')), may hold values from 0.019897461 to 0.5
- gate_act: bfloat16 [4, 128, 384, 768], P('dp', 'expert', None, 'tensor'), may hold values from -8 to 8
- up_act: bfloat16 [4, 128, 384, 768], P('dp', 'expert', None, 'tensor'), may hold values from -6 to 6
- w_down: bfloat16 [128, 768, 4096], P('expert', 'tensor'), may hold values from -0.21875 to 0.21875
Outputs:
- grad_gate: bfloat16 [4, 128, 384, 768], P('dp', 'expert', None, 'tensor')
- grad_up: bfloat16 [4, 128, 384, 768], P('dp', 'expert', None, 'tensor')
- grad_w_down: bfloat16 [128, 768, 4096], P('expert', 'tensor', 'dp')
- grad_probs: float32 [16384, 8], P(('expert', 'dp'))
The draws below stay inside these ranges and needn't reach their ends.
Inputs may be any that keep to these rules, and one draw needn't show every extreme that they name: `route_ids`: each row names 8 different experts. Within the 64 rows of one index pair of expert and dp no expert is named more than 6 times, and in every draw some expert is named exactly 6 times there.
All inputs are finite; a program needn't handle non-finite values.
Results may differ from the reference program's by a relative error of at most 0.009.
Values may be sent and summed in bfloat16 or wider, within the bound.
No kernel may reach another device: no remote copies, remote signals or barrier semaphores. Data moves between devices by JAX's collectives and lax.ppermute only.
A program may use at most 64 MiB of HBM per device.

```python
import math
import jax
import jax.numpy as jnp
import numpy as np
from jax import lax

D = 4096
FF = 768
EXPERTS = 128
TOP = 8
TOK_DEV = 64
CAP = 6
SLOTS = 384
TOKENS = 16384
N_EXPERT = 64
N_DP = 4


def shard_levels(own_key, extent, split, smallest, top_value):
    def one(axis_at, shards_of):
        heights = jax.random.uniform(jax.random.fold_in(jax.random.fold_in(own_key, 6), axis_at), (shards_of,), jnp.float32, smallest / len(split), top_value / len(split))
        return jnp.repeat(jnp.exp(heights), extent[axis_at] // shards_of).reshape((-1,) + (1,) * (len(extent) - axis_at - 1))

    level = one(*split[0])
    for cut in split[1:]:
        level = level * one(*cut)
    return level


def assign_block(rng, own, number, rows, count, top, most, skew):
    order = jax.random.permutation(rng, count)
    packed, ordinary = shares(count, rows * top, most, skew, True), shares(count, rows * top, most, skew, False)
    places = jnp.arange(count)

    def named(lengths, offset_by):
        used = int((lengths > 0).sum())
        fixed = max(1, used // 4)
        passed = fixed + (places - fixed + offset_by * (used - fixed)) % max(1, count - fixed)
        return jnp.zeros((count,), jnp.int32).at[order[jnp.where(places < fixed, places, passed)]].set(jnp.asarray(lengths, jnp.int32))

    lengths = jnp.where(number % 4 == 0, named(packed, number // 4), named(ordinary, number - number // 4 - 1))
    mixed = jax.random.permutation(jax.random.fold_in(own, 3), count)
    donor, receiver = mixed[0:count // 2 * 2:2], mixed[1:count // 2 * 2:2]
    room = jnp.minimum(lengths[donor] - 1, most - lengths[receiver]) // 2
    room = jnp.where((donor == order[0]) | (receiver == order[0]) | (lengths[receiver] == 0), 0, jnp.maximum(room, 0))
    passed = jax.random.randint(jax.random.fold_in(own, 4), (count // 2,), 0, 1 << 20) % (room + 1)
    lengths = lengths.at[donor].add(-passed).at[receiver].add(passed)
    labels = jnp.searchsorted(jnp.cumsum(lengths), jnp.arange(rows * top), side="right").astype(jnp.int32)
    grid = labels.reshape(top, rows).T
    grid = grid[jax.random.permutation(jax.random.fold_in(own, 1), rows)]
    offset_by = jax.random.randint(jax.random.fold_in(own, 2), (rows, 1), 0, top)
    return jnp.take_along_axis(grid, (jnp.arange(top)[None, :] + offset_by) % top, axis=1)


def shares(count, total, most, slope, full):
    portions = [(1 << 20) // math.isqrt(grade ** slope) + 1 for grade in range(1, count + 1)]
    largest = most if full else min(most, max(-(-total // count), total * portions[0] // sum(portions)))
    least = 1 if total - largest >= count - 1 else 0
    holding, rest = [largest] + [least] * (count - 1), total - largest - least * (count - 1)
    while rest > 0:
        candidates = [i for i in range(1, count) if holding[i] < largest] or [i for i in range(1, count) if holding[i] < most]
        whole, budget = sum([portions[i] for i in candidates]), rest
        for i in candidates:
            extra = min(most - holding[i], max(1, budget * portions[i] // whole), rest)
            holding[i] = holding[i] + extra
            rest = rest - extra
    return np.array(holding)


def normal_values(key, extent, spread, most, pieces=(), held_as=jnp.bfloat16):
    loudness = shard_levels(key, extent, pieces, -0.22, 0.18) if pieces else 1.0
    result = jax.random.normal(key, extent, jnp.float32) * spread * loudness
    return jnp.minimum(jnp.maximum(result, -most), most).astype(held_as)


def setup_inputs(seed: int = 0) -> dict:
    seeds = jax.random.split(jax.random.key(seed), 7)
    grad_out = normal_values(seeds[0], (TOKENS, D), 1.0, 6.0, ((0, 256),))
    route_ids_keys = jax.random.split(jax.random.fold_in(seeds[1], 1), TOKENS // TOK_DEV)
    route_ids_turns = jax.random.permutation(jax.random.fold_in(seeds[1], 3), TOKENS // TOK_DEV)
    route_ids = jax.vmap(lambda own, number: assign_block(jax.random.fold_in(seeds[1], 2), own, number, TOK_DEV, EXPERTS, TOP, CAP, 2))(route_ids_keys, route_ids_turns).reshape((TOKENS, TOP))
    route_probs = jnp.clip(jnp.exp(math.log(0.5) - 3.224016 * jax.random.uniform(seeds[2], (TOKENS, TOP), jnp.float32) ** shard_levels(seeds[2], (TOKENS, TOP), ((0, 256),), -0.2, 0.2)), 0.019897461, 0.5).astype(jnp.bfloat16)
    gate_act = normal_values(seeds[3], (N_DP, EXPERTS, SLOTS, FF), 1.5, 8.0, ((0, 4), (1, 64), (3, 4)))
    up_act = normal_values(seeds[4], (N_DP, EXPERTS, SLOTS, FF), 1.0, 6.0, ((0, 4), (1, 64), (3, 4)))
    w_down = normal_values(seeds[5], (EXPERTS, FF, D), FF ** -0.5, 0.21875, ((0, 64), (1, 4)))
    return {"grad_out": grad_out, "route_ids": route_ids, "route_probs": route_probs, "gate_act": gate_act, "up_act": up_act, "w_down": w_down}


def expert_backward(inputs, grad_out):
    slot_token, slot_weight, gate_in, up_in, weight = inputs
    valid = slot_token >= 0
    picked = grad_out[jnp.maximum(slot_token, 0)]
    slot_rows = jnp.where(valid[:, :, None], picked, jnp.zeros_like(picked))
    grad_hidden = jnp.einsum("rsd,fd->rsf", slot_rows.astype(jnp.float32), weight.astype(jnp.float32))
    gate_pre = gate_in.astype(jnp.float32)
    up_pre = up_in.astype(jnp.float32)
    sigmoid_gate = jax.nn.sigmoid(gate_pre)
    silu_gate = gate_pre * sigmoid_gate
    hidden = (silu_gate * up_pre).astype(jnp.bfloat16)
    slot_dot = jnp.sum(grad_hidden * hidden.astype(jnp.float32), axis=2)
    grad_scaled = slot_weight[:, :, None] * grad_hidden
    grad_up = (grad_scaled * silu_gate).astype(jnp.bfloat16)
    grad_gate = (grad_scaled * up_pre * sigmoid_gate * (1.0 + gate_pre * (1.0 - sigmoid_gate))).astype(jnp.bfloat16)
    scaled_rows = (slot_weight[:, :, None] * slot_rows.astype(jnp.float32)).astype(jnp.bfloat16)
    replica_grad = jnp.einsum("rsf,rsd->rfd", hidden.astype(jnp.float32), scaled_rows.astype(jnp.float32))
    rounded = lax.optimization_barrier(replica_grad.astype(jnp.bfloat16))
    grad_weight = jnp.sum(rounded.astype(jnp.float32), axis=0).astype(jnp.bfloat16)
    return grad_gate, grad_up, grad_weight, slot_dot


def reference(grad_out, route_ids, route_probs, gate_act, up_act, w_down):
    block_count = N_EXPERT * N_DP
    route_count = TOK_DEV * TOP
    routes_block = route_ids.reshape(block_count, route_count).astype(jnp.int32)
    matches = (routes_block[:, :, None] == jnp.arange(EXPERTS, dtype=jnp.int32)[None, None, :]).astype(jnp.int32)
    earlier = jnp.cumsum(matches, axis=1) - matches
    position = jnp.sum(earlier * matches, axis=2).astype(jnp.int32)
    block_index = jnp.arange(block_count, dtype=jnp.int32)[:, None]
    source = block_index // N_DP
    replica = jnp.broadcast_to(block_index % N_DP, (block_count, route_count))
    slot = (source * CAP + position).astype(jnp.int32)
    token_index = (block_index * TOK_DEV + jnp.arange(route_count, dtype=jnp.int32)[None, :] // TOP).astype(jnp.int32)
    flat_replica = replica.reshape(-1)
    flat_expert = routes_block.reshape(-1)
    flat_slot = slot.reshape(-1)
    slot_token = jnp.full((N_DP, EXPERTS, SLOTS), -1, jnp.int32).at[flat_replica, flat_expert, flat_slot].set(token_index.reshape(-1))
    slot_weight = jnp.zeros((N_DP, EXPERTS, SLOTS), jnp.float32).at[flat_replica, flat_expert, flat_slot].set(route_probs.reshape(-1).astype(jnp.float32))
    inputs = (jnp.transpose(slot_token, (1, 0, 2)), jnp.transpose(slot_weight, (1, 0, 2)),
              jnp.transpose(gate_act, (1, 0, 2, 3)), jnp.transpose(up_act, (1, 0, 2, 3)), w_down)
    grad_gate, grad_up, grad_w_down, slot_dot = lax.map(lambda item: expert_backward(item, grad_out), inputs)
    grad_gate = jnp.transpose(grad_gate, (1, 0, 2, 3))
    grad_up = jnp.transpose(grad_up, (1, 0, 2, 3))
    slot_dot = jnp.transpose(slot_dot, (1, 0, 2))
    grad_probs = slot_dot[flat_replica, flat_expert, flat_slot].reshape(TOKENS, TOP)
    return (grad_gate, grad_up, grad_w_down, grad_probs)
```

```python
import jax
import jax.numpy as jnp
import numpy as np
from jax import lax
from jax.experimental import pallas as pl
from jax.experimental.pallas import tpu as pltpu
from jax.sharding import PartitionSpec as P

STRIDE = 8
OFFSETS = (0, -1, -2, -3, 1, 2, 3, 4)
SHIFTS = (-4, 3, -3, 2, -2, 1, -1, 0)
VMEM = pltpu.VMEM
LIMIT = 60 * 1024 * 1024


def spec():
    return pl.BlockSpec(memory_space=VMEM)


def call(body, outs, *args, scratch=(), flops=0, moved=0):
    smem = pl.BlockSpec(memory_space=pltpu.SMEM)
    return pl.pallas_call(
        body,
        out_shape=outs,
        in_specs=[smem if a.dtype == jnp.int32 and a.shape == (1,) else spec() for a in args],
        out_specs=jax.tree.map(lambda _: spec(), outs),
        scratch_shapes=list(scratch),
        compiler_params=pltpu.CompilerParams(vmem_limit_bytes=LIMIT),
        cost_estimate=pl.CostEstimate(flops=flops, bytes_accessed=moved, transcendentals=0),
    )(*args)


def dot(a, b):
    return jnp.dot(a, b, preferred_element_type=jnp.float32)


def dot_nt(a, b):
    return lax.dot_general(a, b, (((1,), (1,)), ((), ())), preferred_element_type=jnp.float32)


def earlier_matrix(n, block):
    row = lax.broadcasted_iota(jnp.int32, (n, n), 0)
    col = lax.broadcasted_iota(jnp.int32, (n, n), 1)
    same = (row // block) == (col // block)
    return jnp.where((row < col) & same, 1.0, 0.0).astype(jnp.bfloat16)


def pack_body(t_ref, x_ref, ids_ref, probs_ref, out_ref):
    t = t_ref[0]
    toks = x_ref.shape[0]
    for c in range(8):
        start = pl.multiple_of((c // 2) * 1024 + t * 256 + (c % 2) * 128, 128)
        out_ref[c * toks : (c + 1) * toks, :] = x_ref[:, pl.ds(start, 128)]
    both = jnp.concatenate(
        [ids_ref[...].astype(jnp.float32), probs_ref[...].astype(jnp.float32)], axis=1
    )
    out_ref[8 * toks : 8 * toks + 8, :] = both.astype(jnp.bfloat16)


def select_body(s_ref, onehot_ref, code_ref, exp_ref, *refs):
    blocks, outs = refs[:9], refs[9:]
    s = s_ref[0]
    routes = [b[512:520, :].astype(jnp.float32) for b in blocks[:7]]
    routes.append(blocks[8][256:264, :].astype(jnp.float32))
    ids = jnp.concatenate([r[:, :64] for r in routes], axis=1)
    probs = jnp.concatenate([r[:, 64:] for r in routes], axis=1)
    base = exp_ref[...]
    mine = (2 * s + base) & 127
    mine = mine.astype(jnp.float32)
    match = jnp.zeros((16, 512), jnp.float32)
    prob = jnp.zeros((16, 512), jnp.float32)
    for k in range(8):
        hit = ids[k : k + 1, :] == mine
        match = jnp.where(hit, 1.0, match)
        prob = jnp.where(hit, probs[k : k + 1, :], prob)
    before = earlier_matrix(128, 64)
    low = match.astype(jnp.bfloat16)
    pos = jnp.concatenate(
        [dot(low[:, 128 * c : 128 * (c + 1)], before) for c in range(4)], axis=1
    )
    block = lax.broadcasted_iota(jnp.int32, (16, 512), 1) >> 6
    code = jnp.where(match > 0.0, pos + 6.0 * block.astype(jnp.float32), -1.0)
    onehot = onehot_ref[...]
    spread = dot(onehot, code.astype(jnp.bfloat16))
    chosen = spread == code_ref[...]
    pick = jnp.where(chosen, 1.0, 0.0).astype(jnp.bfloat16)
    weights = dot(onehot, prob.astype(jnp.bfloat16))
    weighted = jnp.where(chosen, weights, 0.0).astype(jnp.bfloat16)
    slot_probs = dot_nt(jnp.ones((8, 512), jnp.bfloat16), weighted).astype(jnp.bfloat16)
    for c in range(8):
        parts = [b[c * 64 : (c + 1) * 64, :] for b in blocks[:7]]
        last = blocks[7] if c < 4 else blocks[8]
        parts.append(last[(c % 4) * 64 : (c % 4 + 1) * 64, :])
        rows = dot(pick, jnp.concatenate(parts, axis=0)).astype(jnp.bfloat16)
        for v in range(8):
            outs[v][c * 96 : (c + 1) * 96, :] = rows[v * 96 : (v + 1) * 96, :]
    for v in range(8):
        for c in range(6):
            outs[v][768 + 8 * c : 776 + 8 * c, :] = slot_probs[:, 128 * c : 128 * (c + 1)]


def expert_body(s_ref, place_ref, *refs):
    pieces = refs[:8]
    w_ref, h_ref = refs[8:10]
    gh_ref, dots_ref, gw_ref, prob_ref = refs[10:14]
    arrived_ref, rows_ref, scaled_ref = refs[14:]
    s = s_ref[0]
    for v in range(8):
        for c in range(8):
            arrived_ref[v * 96 : (v + 1) * 96, c * 128 : (c + 1) * 128] = pieces[v][
                c * 96 : (c + 1) * 96, :
            ]
    lane = lax.broadcasted_iota(jnp.int32, (8, 768), 1)
    probs = jnp.zeros((8, 768), jnp.float32)
    for v in range(8):
        wide = jnp.concatenate(
            [pieces[v][768 + 8 * c : 776 + 8 * c, :] for c in range(6)], axis=1
        ).astype(jnp.float32)
        probs = jnp.where((lane >= v * 96) & (lane < (v + 1) * 96), wide, probs)
    target = ((s + place_ref[0:1, :]) & 63) * 6 + place_ref[1:2, :]
    row = lax.broadcasted_iota(jnp.int32, (768, 768), 0)
    perm = jnp.where(row == target, 1.0, 0.0).astype(jnp.bfloat16)
    low = probs.astype(jnp.bfloat16)
    prob_ref[...] = dot_nt(low, perm)
    column = dot_nt(perm, low)[:, :1]
    for c in range(4):
        part = dot(perm, arrived_ref[:, c * 256 : (c + 1) * 256])
        rows_ref[:, c * 256 : (c + 1) * 256] = part.astype(jnp.bfloat16)
        scaled_ref[:, c * 256 : (c + 1) * 256] = (part * column).astype(jnp.bfloat16)
    for e in range(2):
        total = jnp.zeros((1, 384), jnp.float32)
        for t in range(4):
            part = dot_nt(w_ref[t, e], rows_ref[e * 384 : (e + 1) * 384, :])
            gh_ref[t, e] = part.astype(jnp.bfloat16)
            total += jnp.sum(part * h_ref[t, e].astype(jnp.float32), axis=0, keepdims=True)
        dots_ref[e : e + 1, :] = total
    for e in range(2):
        for t in range(4):
            part = dot(h_ref[t, e], scaled_ref[e * 384 : (e + 1) * 384, :]).astype(jnp.bfloat16)
            for r in range(4):
                gw_ref[r, t, e] = part[:, r * 256 : (r + 1) * 256]


def local_body(prob_ref, gh_ref, gate_ref, up_ref, gg_ref, gu_ref):
    for e in range(2):
        total = gh_ref[0, e].astype(jnp.float32)
        for t in range(1, 4):
            total += gh_ref[t, e].astype(jnp.float32)
        gate = gate_ref[e].astype(jnp.float32)
        up = up_ref[e].astype(jnp.float32)
        sig = jax.nn.sigmoid(gate)
        scaled = prob_ref[0:1, e * 384 : (e + 1) * 384] * total
        gu_ref[e] = (scaled * (gate * sig)).astype(jnp.bfloat16)
        gg_ref[e] = (scaled * up * sig * (1.0 + gate * (1.0 - sig))).astype(jnp.bfloat16)


def lookup_body(ids_ref, table_ref, out_ref):
    experts, capacity = 128, 6
    ids = ids_ref[...]
    expert = lax.broadcasted_iota(jnp.int32, (experts, 64), 0)
    match = jnp.zeros((experts, 64), jnp.float32)
    for k in range(8):
        match = jnp.where(ids[k : k + 1, :] == expert, 1.0, match)
    pos = dot(match.astype(jnp.bfloat16), earlier_matrix(64, 64))
    value = jnp.zeros((experts, 64), jnp.float32)
    for j in range(capacity):
        value = jnp.where(pos == float(j), table_ref[:, j : j + 1], value)
    for k in range(8):
        hit = ids[k : k + 1, :] == expert
        out_ref[k : k + 1, :] = jnp.sum(jnp.where(hit, value, 0.0), axis=0, keepdims=True)


def shifted(x, by, count):
    return lax.ppermute(x, "expert", [(i, (i + by) % count) for i in range(count)])


def on_device(x, ids, probs, gate, up, w):
    bf16, f32, shape = jnp.bfloat16, jnp.float32, jax.ShapeDtypeStruct
    count = lax.axis_size("expert")
    s = lax.axis_index("expert").astype(jnp.int32).reshape(1)
    t = lax.axis_index("tensor").astype(jnp.int32).reshape(1)
    ids_t = ids.T
    gate_t = jnp.transpose(gate[0], (0, 2, 1))
    up_t = jnp.transpose(up[0], (0, 2, 1))

    packed = call(pack_body, shape((520, 128), bf16), t, x, ids_t, probs.T)

    w_send = w.reshape(2, 192, 4, 4, 256).transpose(3, 0, 1, 2, 4).reshape(4, 2, 192, 1024)
    w_all = lax.all_to_all(w_send, "tensor", split_axis=0, concat_axis=0, tiled=True)
    gate_f = gate_t.astype(f32)
    hidden = (gate_f * jax.nn.sigmoid(gate_f) * up_t.astype(f32)).astype(bf16)
    h_send = jnp.broadcast_to(hidden[None], (4, 2, 192, 384))
    h_all = lax.all_to_all(h_send, "tensor", split_axis=0, concat_axis=0, tiled=True)

    blocks = {0: packed}
    for step in (1, 2, 3):
        blocks[-step] = shifted(blocks[1 - step], STRIDE, count)
        blocks[step] = shifted(blocks[step - 1], -STRIDE, count)
    far_low = shifted(blocks[-3][:256], STRIDE, count)
    far_high = shifted(blocks[3][256:], -STRIDE, count)

    row = np.arange(768)
    place = row // 48
    onehot = np.zeros((768, 16), np.float32)
    onehot[row, place] = 1.0
    code = (row % 48).astype(np.float32)[:, None]
    shift = np.array(SHIFTS)
    expert = (2 * shift[:, None] + np.arange(2)[None, :]).reshape(16, 1).astype(np.int32)
    pieces = call(
        select_body,
        [shape((816, 128), bf16)] * 8,
        s,
        jnp.asarray(onehot, bf16),
        jnp.asarray(code),
        jnp.asarray(expert),
        *[blocks[o] for o in OFFSETS[:7]],
        far_low,
        far_high,
        flops=2 * 768 * 512 * 1024,
        moved=4 * 1024 * 1024,
    )
    pieces = [p if j == 0 else shifted(p, j, count) for p, j in zip(pieces, SHIFTS)]

    e, o, j = (row // 48) % 2, (row // 6) % 8, row % 6
    source = STRIDE * np.array(OFFSETS)[o] - shift[row // 96]
    tables = np.zeros((8, 768), np.int32)
    tables[0], tables[1] = source, e * 384 + j
    gh, dots, gw, prob = call(
        expert_body,
        [
            shape((4, 2, 192, 384), bf16),
            shape((2, 384), f32),
            shape((4, 4, 2, 192, 256), bf16),
            shape((8, 768), f32),
        ],
        s,
        jnp.asarray(tables),
        *pieces,
        w_all,
        h_all,
        scratch=[VMEM((768, 1024), bf16)] * 3,
        flops=6 * 10**9,
        moved=12 * 1024 * 1024,
    )

    gw_all = lax.all_to_all(gw, "dp", split_axis=0, concat_axis=0, tiled=True)
    gh_all = lax.all_to_all(gh, "tensor", split_axis=0, concat_axis=0, tiled=True)
    cells = jnp.transpose(dots.reshape(2, count, 6), (1, 0, 2)).reshape(count, 12)
    cells = jnp.broadcast_to(cells[None], (4, count, 12)).reshape(4 * count, 12)
    back = lax.all_to_all(cells, ("tensor", "expert"), split_axis=0, concat_axis=0, tiled=True)
    table = back.reshape(4, 2 * count, 6).sum(axis=0)

    grad_gate, grad_up = call(
        local_body,
        [shape((2, 192, 384), bf16)] * 2,
        prob,
        gh_all,
        gate_t,
        up_t,
        flops=10**7,
        moved=4 * 1024 * 1024,
    )
    grad_probs = call(lookup_body, shape((8, 64), f32), ids_t, table).T
    summed = gw_all.astype(f32).sum(axis=0).astype(bf16)
    mine = lax.all_to_all(summed, "tensor", split_axis=0, concat_axis=0, tiled=True)
    grad_w = jnp.transpose(mine, (1, 2, 0, 3)).reshape(2, 192, 1024)
    return (
        jnp.transpose(grad_gate, (0, 2, 1))[None],
        jnp.transpose(grad_up, (0, 2, 1))[None],
        grad_w,
        grad_probs,
    )


def solution(mesh):
    act = P("dp", "expert", None, "tensor")
    tok = P(("expert", "dp"), None)
    return jax.shard_map(
        on_device,
        mesh=mesh,
        in_specs=(tok, tok, tok, act, act, P("expert", "tensor", None)),
        out_specs=(act, act, P("expert", "tensor", "dp"), tok),
        check_vma=False,
    )
```

```python
import jax
import jax.numpy as jnp
import numpy as np
from jax import lax
from jax.experimental import pallas as pl
from jax.experimental.pallas import tpu as pltpu
from jax.sharding import PartitionSpec as P


STRIDE = 8
OFFSETS = (0, -1, -2, -3, 1, 2, 3, 4)
SHIFTS = (-4, 3, -3, 2, -2, 1, -1, 0)
VMEM = pltpu.VMEM
LIMIT = 60 * 1024 * 1024


def spec():
    return pl.BlockSpec(memory_space=VMEM)


def call(body, outs, *args, scratch=(), untouched=(), flops=10**6, moved=10**6):
    smem = pl.BlockSpec(memory_space=pltpu.SMEM)
    specs = [smem if a.dtype == jnp.int32 and a.shape == (3,) else spec() for a in args]
    for i in untouched:
        specs[i] = pl.BlockSpec(memory_space=pl.ANY)
    return pl.pallas_call(
        body,
        out_shape=outs,
        in_specs=specs,
        out_specs=jax.tree.map(lambda _: spec(), outs),
        scratch_shapes=list(scratch),
        compiler_params=pltpu.CompilerParams(vmem_limit_bytes=LIMIT),
        cost_estimate=pl.CostEstimate(flops=flops, bytes_accessed=moved, transcendentals=0),
    )(*args)


def dot(a, b):
    return jnp.dot(a, b, preferred_element_type=jnp.float32)


def dot_nt(a, b):
    return lax.dot_general(a, b, (((1,), (1,)), ((), ())), preferred_element_type=jnp.float32)


def earlier_matrix(n, block):
    row = lax.broadcasted_iota(jnp.int32, (n, n), 0)
    col = lax.broadcasted_iota(jnp.int32, (n, n), 1)
    same = (row // block) == (col // block)
    return jnp.where((row < col) & same, 1.0, 0.0).astype(jnp.bfloat16)


def pack_body(self_ref, x_ref, ids_ref, probs_ref, out_ref):
    t = self_ref[1]
    toks = x_ref.shape[0]
    for c in range(8):
        start = pl.multiple_of((c // 2) * 1024 + t * 256 + (c % 2) * 128, 128)
        out_ref[c * toks : (c + 1) * toks, :] = x_ref[:, pl.ds(start, 128)]
    both = jnp.concatenate(
        [ids_ref[...].astype(jnp.float32), probs_ref[...].astype(jnp.float32)], axis=1
    )
    out_ref[8 * toks : 8 * toks + 8, :] = both.astype(jnp.bfloat16)


def prepare_body(w_ref, gate_ref, up_ref, _, out_ref):
    for e in range(2):
        gate = gate_ref[e].astype(jnp.float32)
        hidden = (gate * jax.nn.sigmoid(gate) * up_ref[e].astype(jnp.float32)).astype(jnp.bfloat16)
        for t in range(4):
            for r in range(4):
                start = r * 1024 + t * 256
                out_ref[t, e, :, r * 256 : (r + 1) * 256] = w_ref[e, :, start : start + 256]
            out_ref[t, e, :, 1024:1408] = hidden


def select_body(self_ref, onehot_ref, code_ref, exp_ref, *refs):
    blocks, outs = refs[:9], refs[9:]
    s = self_ref[0]
    routes = [b[512:520, :].astype(jnp.float32) for b in blocks[:7]]
    routes.append(blocks[8][256:264, :].astype(jnp.float32))
    ids = jnp.concatenate([r[:, :64] for r in routes], axis=1)
    probs = jnp.concatenate([r[:, 64:] for r in routes], axis=1)
    base = exp_ref[...]
    mine = (2 * s + base) & 127
    mine = mine.astype(jnp.float32)
    match = jnp.zeros((16, 512), jnp.float32)
    prob = jnp.zeros((16, 512), jnp.float32)
    for k in range(8):
        hit = ids[k : k + 1, :] == mine
        match = jnp.where(hit, 1.0, match)
        prob = jnp.where(hit, probs[k : k + 1, :], prob)
    before = earlier_matrix(128, 64)
    low = match.astype(jnp.bfloat16)
    pos = jnp.concatenate(
        [dot(low[:, 128 * c : 128 * (c + 1)], before) for c in range(4)], axis=1
    )
    block = lax.broadcasted_iota(jnp.int32, (16, 512), 1) >> 6
    code = jnp.where(match > 0.0, pos + 6.0 * block.astype(jnp.float32), -1.0)
    onehot = onehot_ref[...]
    spread = dot(onehot, code.astype(jnp.bfloat16))
    chosen = spread == code_ref[...]
    pick = jnp.where(chosen, 1.0, 0.0).astype(jnp.bfloat16)
    weights = dot(onehot, prob.astype(jnp.bfloat16))
    weighted = jnp.where(chosen, weights, 0.0).astype(jnp.bfloat16)
    slot_probs = dot_nt(jnp.ones((8, 512), jnp.bfloat16), weighted).astype(jnp.bfloat16)
    for c in range(8):
        parts = [b[c * 64 : (c + 1) * 64, :] for b in blocks[:7]]
        last = blocks[7] if c < 4 else blocks[8]
        parts.append(last[(c % 4) * 64 : (c % 4 + 1) * 64, :])
        rows = dot(pick, jnp.concatenate(parts, axis=0)).astype(jnp.bfloat16)
        for v in range(8):
            for e in range(2):
                outs[v][c * 96 + e * 48 : c * 96 + (e + 1) * 48, :] = rows[
                    e * 384 + v * 48 : e * 384 + (v + 1) * 48, :
                ]
    for v in range(8):
        for c in range(6):
            outs[v][768 + 8 * c : 776 + 8 * c, :] = slot_probs[:, 128 * c : 128 * (c + 1)]


def expert_body(self_ref, place_ref, *refs):
    pieces = refs[:8]
    wh_ref = refs[8]
    gh_refs, gw_refs = refs[9:13], refs[13:17]
    dots_ref, prob_ref = refs[17:19]
    arrived_ref, rows_ref, scaled_ref = refs[19:]
    s, t, r = self_ref[0], self_ref[1], self_ref[2]
    for v in range(8):
        for c in range(8):
            for e in range(2):
                arrived_ref[
                    e * 384 + v * 48 : e * 384 + (v + 1) * 48, c * 128 : (c + 1) * 128
                ] = pieces[v][c * 96 + e * 48 : c * 96 + (e + 1) * 48, :]
    lane = lax.broadcasted_iota(jnp.int32, (8, 768), 1)
    probs = jnp.zeros((8, 768), jnp.float32)
    for v in range(8):
        wide = jnp.concatenate(
            [pieces[v][768 + 8 * c : 776 + 8 * c, :] for c in range(6)], axis=1
        ).astype(jnp.float32)
        mine = place_ref[2:3, :] == v
        probs = jnp.where(mine, wide, probs)
    low = probs.astype(jnp.bfloat16)
    target = ((s + place_ref[0:1, :]) & 63) * 6 + place_ref[1:2, :]
    row = lax.broadcasted_iota(jnp.int32, (384, 384), 0)
    for e in range(2):
        perm = jnp.where(row == target[:, e * 384 : (e + 1) * 384], 1.0, 0.0).astype(jnp.bfloat16)
        mine = low[:, e * 384 : (e + 1) * 384]
        prob_ref[:, e * 384 : (e + 1) * 384] = dot_nt(mine, perm)
        column = dot_nt(perm, mine)[:, :1]
        here = slice(e * 384, (e + 1) * 384)
        for c in range(4):
            part = dot(perm, arrived_ref[here, c * 256 : (c + 1) * 256])
            rows_ref[here, c * 256 : (c + 1) * 256] = part.astype(jnp.bfloat16)
            scaled_ref[here, c * 256 : (c + 1) * 256] = (part * column).astype(jnp.bfloat16)
    for e in range(2):
        hidden = jnp.concatenate([wh_ref[k, e, :, 1024:1408] for k in range(4)], axis=0)
        for rho in range(4):
            start = pl.multiple_of(((r + rho) & 3) * 256, 256)
            part = dot(hidden, scaled_ref[e * 384 : (e + 1) * 384, pl.ds(start, 256)])
            part = part.astype(jnp.bfloat16)
            for k in range(4):
                gw_refs[rho][k, e] = part[k * 192 : (k + 1) * 192, :]
    for e in range(2):
        total = jnp.zeros((1, 384), jnp.float32)
        for delta in range(4):
            k = (t + delta) & 3
            part = dot_nt(wh_ref[k, e, :, :1024], rows_ref[e * 384 : (e + 1) * 384, :])
            gh_refs[delta][e] = part.astype(jnp.bfloat16)
            hidden = wh_ref[k, e, :, 1024:1408].astype(jnp.float32)
            total += jnp.sum(part * hidden, axis=0, keepdims=True)
        dots_ref[e : e + 1, :] = total


def local_body(prob_ref, *refs):
    gh_refs, gate_ref, up_ref, gg_ref, gu_ref = refs[:4], *refs[4:]
    for e in range(2):
        total = gh_refs[0][e].astype(jnp.float32)
        for k in range(1, 4):
            total += gh_refs[k][e].astype(jnp.float32)
        gate = gate_ref[e].astype(jnp.float32)
        up = up_ref[e].astype(jnp.float32)
        sig = jax.nn.sigmoid(gate)
        scaled = prob_ref[0:1, e * 384 : (e + 1) * 384] * total
        gu_ref[e] = (scaled * (gate * sig)).astype(jnp.bfloat16)
        gg_ref[e] = (scaled * up * sig * (1.0 + gate * (1.0 - sig))).astype(jnp.bfloat16)


def replica_body(self_ref, *refs):
    parts, outs = refs[:4], refs[4:]
    for delta in range(4):
        k = (self_ref[1] + delta) & 3
        for e in range(2):
            total = parts[0][k, e].astype(jnp.float32)
            for part in parts[1:]:
                total += part[k, e].astype(jnp.float32)
            outs[delta][e] = total.astype(jnp.bfloat16)


def place_body(self_ref, *refs):
    parts, out_ref = refs[:4], refs[4]
    for delta in range(4):
        start = pl.multiple_of(((self_ref[1] - delta) & 3) * 256, 256)
        for e in range(2):
            out_ref[e, :, pl.ds(start, 256)] = parts[delta][e]


def lookup_body(ids_ref, table_ref, out_ref):
    experts, capacity = 128, 6
    ids = ids_ref[...]
    expert = lax.broadcasted_iota(jnp.int32, (experts, 64), 0)
    match = jnp.zeros((experts, 64), jnp.float32)
    for k in range(8):
        match = jnp.where(ids[k : k + 1, :] == expert, 1.0, match)
    pos = dot(match.astype(jnp.bfloat16), earlier_matrix(64, 64))
    value = jnp.zeros((experts, 64), jnp.float32)
    for j in range(capacity):
        value = jnp.where(pos == float(j), table_ref[:, j : j + 1], value)
    for k in range(8):
        hit = ids[k : k + 1, :] == expert
        out_ref[k : k + 1, :] = jnp.sum(jnp.where(hit, value, 0.0), axis=0, keepdims=True)


def shifted(x, by, axis):
    count = lax.axis_size(axis)
    return lax.ppermute(x, axis, [(i, (i + by) % count) for i in range(count)])


def spread(parts, axis):
    return [parts[0], *(shifted(parts[d], d, axis) for d in (1, 2, 3))]


def slot_tables():
    row = np.arange(768)
    onehot = np.zeros((768, 16), np.float32)
    onehot[row, row // 48] = 1.0
    code = (row % 48).astype(np.float32)[:, None]
    shift = np.array(SHIFTS)
    expert = (2 * shift[None, :] + np.arange(2)[:, None]).reshape(16, 1).astype(np.int32)
    piece, o, j = (row % 384) // 48, (row // 6) % 8, row % 6
    tables = np.zeros((8, 768), np.int32)
    tables[0] = STRIDE * np.array(OFFSETS)[o] - shift[piece]
    tables[1] = j
    tables[2] = piece
    return onehot, code, expert, tables


def backward(x, ids, probs, gate, up, w):
    bf16, f32, shape = jnp.bfloat16, jnp.float32, jax.ShapeDtypeStruct
    count = lax.axis_size("expert")
    own = jnp.stack([lax.axis_index(a).astype(jnp.int32) for a in ("expert", "tensor", "dp")])
    ids_t = ids.T
    gate_t = jnp.transpose(gate[0], (0, 2, 1))
    up_t = jnp.transpose(up[0], (0, 2, 1))

    packed = call(pack_body, shape((520, 128), bf16), own, x, ids_t, probs.T)
    blocks = {0: packed}
    for step in (1, 2, 3):
        blocks[-step] = shifted(blocks[1 - step], STRIDE, "expert")
        blocks[step] = shifted(blocks[step - 1], -STRIDE, "expert")
    far_low = shifted(blocks[-3][:256], STRIDE, "expert")
    far_high = shifted(blocks[3][256:], -STRIDE, "expert")

    to_send = call(
        prepare_body,
        shape((4, 2, 192, 1408), bf16),
        w,
        gate_t,
        up_t,
        blocks[-1],
        untouched=(3,),
        flops=10**7,
        moved=8 * 1024 * 1024,
    )
    wh_all = lax.all_to_all(to_send, "tensor", split_axis=0, concat_axis=0, tiled=True)

    onehot, code, expert, tables = slot_tables()
    pieces = call(
        select_body,
        [shape((816, 128), bf16)] * 8,
        own,
        jnp.asarray(onehot, bf16),
        jnp.asarray(code),
        jnp.asarray(expert),
        *[blocks[o] for o in OFFSETS[:7]],
        far_low,
        far_high,
        flops=2 * 768 * 512 * 1024,
        moved=4 * 1024 * 1024,
    )
    pieces = [p if j == 0 else shifted(p, j, "expert") for p, j in zip(pieces, SHIFTS)]

    results = call(
        expert_body,
        [shape((2, 192, 384), bf16)] * 4
        + [shape((4, 2, 192, 256), bf16)] * 4
        + [shape((2, 384), f32), shape((8, 768), f32)],
        own,
        jnp.asarray(tables),
        *pieces,
        wh_all,
        scratch=[VMEM((768, 1024), bf16)] * 3,
        flops=6 * 10**9,
        moved=12 * 1024 * 1024,
    )
    gh, gw, dots, prob = results[:4], results[4:8], results[8], results[9]

    gw = spread(gw, "dp")
    gh = spread(gh, "tensor")
    cells = jnp.transpose(dots.reshape(2, count, 6), (1, 0, 2)).reshape(count, 12)
    cells = jnp.broadcast_to(cells[None], (4, count, 12)).reshape(4 * count, 12)
    back = lax.all_to_all(cells, ("tensor", "expert"), split_axis=0, concat_axis=0, tiled=True)
    table = back.reshape(4, 2 * count, 6).sum(axis=0)

    summed = call(replica_body, [shape((2, 192, 256), bf16)] * 4, own, *gw, moved=4 * 1024 * 1024, flops=10**7)
    summed = spread(summed, "tensor")
    grad_gate, grad_up = call(
        local_body,
        [shape((2, 192, 384), bf16)] * 2,
        prob,
        *gh,
        gate_t,
        up_t,
        flops=10**7,
        moved=4 * 1024 * 1024,
    )
    grad_w = call(place_body, shape((2, 192, 1024), bf16), own, *summed, moved=2 * 1024 * 1024, flops=10**6)
    grad_probs = call(lookup_body, shape((8, 64), f32), ids_t, table, flops=10**6, moved=10**5).T
    return (
        jnp.transpose(grad_gate, (0, 2, 1))[None],
        jnp.transpose(grad_up, (0, 2, 1))[None],
        grad_w,
        grad_probs,
    )


def solution(mesh):
    act = P("dp", "expert", None, "tensor")
    tok = P(("expert", "dp"), None)
    return jax.shard_map(
        backward,
        mesh=mesh,
        in_specs=(tok, tok, tok, act, act, P("expert", "tensor", None)),
        out_specs=(act, act, P("expert", "tensor", "dp"), tok),
        check_vma=False,
    )
```

```python
import jax
import jax.numpy as jnp
import numpy as np
from jax import lax
from jax.experimental import pallas as pl
from jax.experimental.pallas import tpu as pltpu
from jax.sharding import PartitionSpec as P


STRIDE = 8
OFFSETS = (0, -1, -2, -3, 1, 2, 3, 4)
SHIFTS = (-4, 3, -3, 2, -2, 1, -1, 0)
VMEM = pltpu.VMEM
LIMIT = 60 * 1024 * 1024


def spec():
    return pl.BlockSpec(memory_space=VMEM)


def call(body, outs, *args, scratch=(), untouched=(), flops=10**6, moved=10**6):
    smem = pl.BlockSpec(memory_space=pltpu.SMEM)
    specs = [smem if a.dtype == jnp.int32 and a.shape == (3,) else spec() for a in args]
    for i in untouched:
        specs[i] = pl.BlockSpec(memory_space=pl.ANY)
    return pl.pallas_call(
        body,
        out_shape=outs,
        in_specs=specs,
        out_specs=jax.tree.map(lambda _: spec(), outs),
        scratch_shapes=list(scratch),
        compiler_params=pltpu.CompilerParams(vmem_limit_bytes=LIMIT),
        cost_estimate=pl.CostEstimate(flops=flops, bytes_accessed=moved, transcendentals=0),
    )(*args)


def dot(a, b):
    return jnp.dot(a, b, preferred_element_type=jnp.float32)


def dot_nt(a, b):
    return lax.dot_general(a, b, (((1,), (1,)), ((), ())), preferred_element_type=jnp.float32)


def way(self_ref):
    return 1 - 2 * (self_ref[0] & 1)


def earlier_matrix(n, block):
    row = lax.broadcasted_iota(jnp.int32, (n, n), 0)
    col = lax.broadcasted_iota(jnp.int32, (n, n), 1)
    same = (row // block) == (col // block)
    return jnp.where((row < col) & same, 1.0, 0.0).astype(jnp.bfloat16)


def pack_body(self_ref, x_ref, ids_ref, probs_ref, out_ref):
    t = self_ref[1]
    toks = x_ref.shape[0]
    for c in range(8):
        start = pl.multiple_of((c // 2) * 1024 + t * 256 + (c % 2) * 128, 128)
        out_ref[c * toks : (c + 1) * toks, :] = x_ref[:, pl.ds(start, 128)]
    both = jnp.concatenate(
        [ids_ref[...].astype(jnp.float32), probs_ref[...].astype(jnp.float32)], axis=1
    )
    out_ref[8 * toks : 8 * toks + 8, :] = both.astype(jnp.bfloat16)


def prepare_body(w_ref, gate_ref, up_ref, _, out_ref):
    for e in range(2):
        gate = gate_ref[e].astype(jnp.float32)
        hidden = (gate * jax.nn.sigmoid(gate) * up_ref[e].astype(jnp.float32)).astype(jnp.bfloat16)
        for t in range(4):
            for r in range(4):
                start = r * 1024 + t * 256
                out_ref[t, e, :, r * 256 : (r + 1) * 256] = w_ref[e, :, start : start + 256]
            out_ref[t, e, :, 1024:1408] = hidden


def select_body(self_ref, onehot_ref, code_ref, exp_ref, *refs):
    blocks, outs = refs[:9], refs[9:]
    s = self_ref[0]
    routes = [b[512:520, :].astype(jnp.float32) for b in blocks[:7]]
    routes.append(blocks[8][256:264, :].astype(jnp.float32))
    ids = jnp.concatenate([r[:, :64] for r in routes], axis=1)
    probs = jnp.concatenate([r[:, 64:] for r in routes], axis=1)
    mine = (2 * (s + way(self_ref) * exp_ref[:, :1]) + exp_ref[:, 1:2]) & 127
    mine = mine.astype(jnp.float32)
    match = jnp.zeros((16, 512), jnp.float32)
    prob = jnp.zeros((16, 512), jnp.float32)
    for k in range(8):
        hit = ids[k : k + 1, :] == mine
        match = jnp.where(hit, 1.0, match)
        prob = jnp.where(hit, probs[k : k + 1, :], prob)
    before = earlier_matrix(128, 64)
    low = match.astype(jnp.bfloat16)
    pos = jnp.concatenate(
        [dot(low[:, 128 * c : 128 * (c + 1)], before) for c in range(4)], axis=1
    )
    block = lax.broadcasted_iota(jnp.int32, (16, 512), 1) >> 6
    code = jnp.where(match > 0.0, pos + 6.0 * block.astype(jnp.float32), -1.0)
    onehot = onehot_ref[...]
    spread = dot(onehot, code.astype(jnp.bfloat16))
    chosen = spread == code_ref[...]
    pick = jnp.where(chosen, 1.0, 0.0).astype(jnp.bfloat16)
    weights = dot(onehot, prob.astype(jnp.bfloat16))
    weighted = jnp.where(chosen, weights, 0.0).astype(jnp.bfloat16)
    slot_probs = dot_nt(jnp.ones((8, 512), jnp.bfloat16), weighted).astype(jnp.bfloat16)
    for c in range(8):
        parts = [b[c * 64 : (c + 1) * 64, :] for b in blocks[:7]]
        last = blocks[7] if c < 4 else blocks[8]
        parts.append(last[(c % 4) * 64 : (c % 4 + 1) * 64, :])
        rows = dot(pick, jnp.concatenate(parts, axis=0)).astype(jnp.bfloat16)
        for v in range(8):
            for e in range(2):
                outs[v][c * 96 + e * 48 : c * 96 + (e + 1) * 48, :] = rows[
                    e * 384 + v * 48 : e * 384 + (v + 1) * 48, :
                ]
    for v in range(8):
        for c in range(6):
            outs[v][768 + 8 * c : 776 + 8 * c, :] = slot_probs[:, 128 * c : 128 * (c + 1)]


def expert_body(self_ref, place_ref, *refs):
    pieces = refs[:8]
    wh_ref = refs[8]
    gh_refs, gw_refs = refs[9:13], refs[13:17]
    dots_ref, prob_ref = refs[17:19]
    arrived_ref, rows_ref, scaled_ref = refs[19:]
    s, t, r = self_ref[0], self_ref[1], self_ref[2]
    turn = way(self_ref)
    for v in range(8):
        for c in range(8):
            for e in range(2):
                arrived_ref[
                    e * 384 + v * 48 : e * 384 + (v + 1) * 48, c * 128 : (c + 1) * 128
                ] = pieces[v][c * 96 + e * 48 : c * 96 + (e + 1) * 48, :]
    lane = lax.broadcasted_iota(jnp.int32, (8, 768), 1)
    probs = jnp.zeros((8, 768), jnp.float32)
    for v in range(8):
        wide = jnp.concatenate(
            [pieces[v][768 + 8 * c : 776 + 8 * c, :] for c in range(6)], axis=1
        ).astype(jnp.float32)
        mine = place_ref[2:3, :] == v
        probs = jnp.where(mine, wide, probs)
    low = probs.astype(jnp.bfloat16)
    sign = 1 - 2 * ((s + place_ref[3:4, :]) & 1)
    target = ((s + sign * place_ref[0:1, :]) & 63) * 6 + place_ref[1:2, :]
    row = lax.broadcasted_iota(jnp.int32, (384, 384), 0)
    for e in range(2):
        perm = jnp.where(row == target[:, e * 384 : (e + 1) * 384], 1.0, 0.0).astype(jnp.bfloat16)
        mine = low[:, e * 384 : (e + 1) * 384]
        prob_ref[:, e * 384 : (e + 1) * 384] = dot_nt(mine, perm)
        column = dot_nt(perm, mine)[:, :1]
        here = slice(e * 384, (e + 1) * 384)
        for c in range(4):
            part = dot(perm, arrived_ref[here, c * 256 : (c + 1) * 256])
            rows_ref[here, c * 256 : (c + 1) * 256] = part.astype(jnp.bfloat16)
            scaled_ref[here, c * 256 : (c + 1) * 256] = (part * column).astype(jnp.bfloat16)
    for e in range(2):
        hidden = jnp.concatenate([wh_ref[k, e, :, 1024:1408] for k in range(4)], axis=0)
        for rho in range(4):
            start = pl.multiple_of(((r + turn * rho) & 3) * 256, 256)
            part = dot(hidden, scaled_ref[e * 384 : (e + 1) * 384, pl.ds(start, 256)])
            part = part.astype(jnp.bfloat16)
            for k in range(4):
                gw_refs[rho][k, e] = part[k * 192 : (k + 1) * 192, :]
    for e in range(2):
        total = jnp.zeros((1, 384), jnp.float32)
        for delta in range(4):
            k = (t + turn * delta) & 3
            part = dot_nt(wh_ref[k, e, :, :1024], rows_ref[e * 384 : (e + 1) * 384, :])
            gh_refs[delta][e] = part.astype(jnp.bfloat16)
            hidden = wh_ref[k, e, :, 1024:1408].astype(jnp.float32)
            total += jnp.sum(part * hidden, axis=0, keepdims=True)
        dots_ref[e : e + 1, :] = total


def local_body(prob_ref, *refs):
    gh_refs, gate_ref, up_ref, gg_ref, gu_ref = refs[:4], *refs[4:]
    for e in range(2):
        total = gh_refs[0][e].astype(jnp.float32)
        for k in range(1, 4):
            total += gh_refs[k][e].astype(jnp.float32)
        gate = gate_ref[e].astype(jnp.float32)
        up = up_ref[e].astype(jnp.float32)
        sig = jax.nn.sigmoid(gate)
        scaled = prob_ref[0:1, e * 384 : (e + 1) * 384] * total
        gu_ref[e] = (scaled * (gate * sig)).astype(jnp.bfloat16)
        gg_ref[e] = (scaled * up * sig * (1.0 + gate * (1.0 - sig))).astype(jnp.bfloat16)


def replica_body(self_ref, *refs):
    parts, outs = refs[:4], refs[4:]
    for delta in range(4):
        k = (self_ref[1] + way(self_ref) * delta) & 3
        for e in range(2):
            total = parts[0][k, e].astype(jnp.float32)
            for part in parts[1:]:
                total += part[k, e].astype(jnp.float32)
            outs[delta][e] = total.astype(jnp.bfloat16)


def place_body(self_ref, *refs):
    parts, out_ref = refs[:4], refs[4]
    for delta in range(4):
        start = pl.multiple_of(((self_ref[1] - way(self_ref) * delta) & 3) * 256, 256)
        for e in range(2):
            out_ref[e, :, pl.ds(start, 256)] = parts[delta][e]


def lookup_body(ids_ref, table_ref, out_ref):
    experts, capacity = 128, 6
    ids = ids_ref[...]
    expert = lax.broadcasted_iota(jnp.int32, (experts, 64), 0)
    match = jnp.zeros((experts, 64), jnp.float32)
    for k in range(8):
        match = jnp.where(ids[k : k + 1, :] == expert, 1.0, match)
    pos = dot(match.astype(jnp.bfloat16), earlier_matrix(64, 64))
    value = jnp.zeros((experts, 64), jnp.float32)
    for j in range(capacity):
        value = jnp.where(pos == float(j), table_ref[:, j : j + 1], value)
    for k in range(8):
        hit = ids[k : k + 1, :] == expert
        out_ref[k : k + 1, :] = jnp.sum(jnp.where(hit, value, 0.0), axis=0, keepdims=True)


def shifted(x, by, axis):
    count, others = lax.axis_size(axis), lax.axis_size("expert")
    if axis == "expert":
        axes, pairs = axis, [(i, (i + by * (1 - 2 * (i & 1))) % count) for i in range(count)]
    else:
        major = axis == "tensor"
        axes = (axis, "expert") if major else ("expert", axis)

        def at(s, i):
            return i * others + s if major else s * count + i

        pairs = [
            (at(s, i), at(s, (i + by * (1 - 2 * (s & 1))) % count))
            for s in range(others)
            for i in range(count)
        ]
    return lax.ppermute(x, axes, pairs)


def spread(parts, axis):
    return [parts[0], *(shifted(parts[d], d, axis) for d in (1, 2, 3))]


def slot_tables():
    row = np.arange(768)
    onehot = np.zeros((768, 16), np.float32)
    onehot[row, row // 48] = 1.0
    code = (row % 48).astype(np.float32)[:, None]
    shift = np.array(SHIFTS)
    expert = np.stack([np.tile(shift, 2), np.repeat(np.arange(2), 8)], axis=1).astype(np.int32)
    piece, o, j = (row % 384) // 48, (row // 6) % 8, row % 6
    tables = np.zeros((8, 768), np.int32)
    tables[0] = STRIDE * np.array(OFFSETS)[o] - shift[piece]
    tables[1] = j
    tables[2] = piece
    tables[3] = shift[piece] & 1
    return onehot, code, expert, tables


def backward(x, ids, probs, gate, up, w):
    bf16, f32, shape = jnp.bfloat16, jnp.float32, jax.ShapeDtypeStruct
    count = lax.axis_size("expert")
    own = jnp.stack([lax.axis_index(a).astype(jnp.int32) for a in ("expert", "tensor", "dp")])
    ids_t = ids.T
    gate_t = jnp.transpose(gate[0], (0, 2, 1))
    up_t = jnp.transpose(up[0], (0, 2, 1))

    packed = call(pack_body, shape((520, 128), bf16), own, x, ids_t, probs.T)
    blocks = {0: packed}
    for step in (1, 2, 3):
        blocks[-step] = shifted(blocks[1 - step], STRIDE, "expert")
        blocks[step] = shifted(blocks[step - 1], -STRIDE, "expert")
    far_low = shifted(blocks[-3][:256], STRIDE, "expert")
    far_high = shifted(blocks[3][256:], -STRIDE, "expert")

    to_send = call(
        prepare_body,
        shape((4, 2, 192, 1408), bf16),
        w,
        gate_t,
        up_t,
        packed,
        untouched=(3,),
        flops=10**7,
        moved=8 * 1024 * 1024,
    )
    wh_all = lax.all_to_all(to_send, "tensor", split_axis=0, concat_axis=0, tiled=True)

    onehot, code, expert, tables = slot_tables()
    pieces = call(
        select_body,
        [shape((816, 128), bf16)] * 8,
        own,
        jnp.asarray(onehot, bf16),
        jnp.asarray(code),
        jnp.asarray(expert),
        *[blocks[o] for o in OFFSETS[:7]],
        far_low,
        far_high,
        flops=2 * 768 * 512 * 1024,
        moved=4 * 1024 * 1024,
    )
    pieces = [p if j == 0 else shifted(p, j, "expert") for p, j in zip(pieces, SHIFTS)]

    results = call(
        expert_body,
        [shape((2, 192, 384), bf16)] * 4
        + [shape((4, 2, 192, 256), bf16)] * 4
        + [shape((2, 384), f32), shape((8, 768), f32)],
        own,
        jnp.asarray(tables),
        *pieces,
        wh_all,
        scratch=[VMEM((768, 1024), bf16)] * 3,
        flops=6 * 10**9,
        moved=12 * 1024 * 1024,
    )
    gh, gw, dots, prob = results[:4], results[4:8], results[8], results[9]

    gw = spread(gw, "dp")
    gh = spread(gh, "tensor")
    cells = jnp.transpose(dots.reshape(2, count, 6), (1, 0, 2)).reshape(count, 12)
    cells = jnp.broadcast_to(cells[None], (4, count, 12)).reshape(4 * count, 12)
    back = lax.all_to_all(cells, ("tensor", "expert"), split_axis=0, concat_axis=0, tiled=True)
    table = back.reshape(4, 2 * count, 6).sum(axis=0)

    summed = call(replica_body, [shape((2, 192, 256), bf16)] * 4, own, *gw, moved=4 * 1024 * 1024, flops=10**7)
    summed = spread(summed, "tensor")
    grad_gate, grad_up = call(
        local_body,
        [shape((2, 192, 384), bf16)] * 2,
        prob,
        *gh,
        gate_t,
        up_t,
        flops=10**7,
        moved=4 * 1024 * 1024,
    )
    grad_w = call(place_body, shape((2, 192, 1024), bf16), own, *summed, moved=2 * 1024 * 1024, flops=10**6)
    grad_probs = call(lookup_body, shape((8, 64), f32), ids_t, table, flops=10**6, moved=10**5).T
    return (
        jnp.transpose(grad_gate, (0, 2, 1))[None],
        jnp.transpose(grad_up, (0, 2, 1))[None],
        grad_w,
        grad_probs,
    )


def solution(mesh):
    act = P("dp", "expert", None, "tensor")
    tok = P(("expert", "dp"), None)
    return jax.shard_map(
        backward,
        mesh=mesh,
        in_specs=(tok, tok, tok, act, act, P("expert", "tensor", None)),
        out_specs=(act, act, P("expert", "tensor", "dp"), tok),
        check_vma=False,
    )
```

```python
import jax
import jax.numpy as jnp
import numpy as np
from jax import lax
from jax.experimental import pallas as pl
from jax.experimental.pallas import tpu as pltpu
from jax.sharding import PartitionSpec as P


STRIDE = 8
OFFSETS = (0, -1, -2, -3, 1, 2, 3, 4)
SHIFTS = (-4, 3, -3, 2, -2, 1, -1, 0)
VMEM = pltpu.VMEM


def spec():
    return pl.BlockSpec(memory_space=VMEM)


def call(body, outs, *args, scratch=(), untouched=(), far_outs=0, aliases=None, flops=10**6, moved=10**6, mib=60):
    smem = pl.BlockSpec(memory_space=pltpu.SMEM)
    specs = [smem if a.dtype == jnp.int32 and a.shape == (3,) else spec() for a in args]
    out_specs = jax.tree.map(lambda _: spec(), outs)
    for i in range(far_outs):
        out_specs[i] = pl.BlockSpec(memory_space=pltpu.HBM)
    for i in untouched:
        specs[i] = pl.BlockSpec(memory_space=pl.ANY)
    return pl.pallas_call(
        body,
        out_shape=outs,
        in_specs=specs,
        out_specs=out_specs,
        scratch_shapes=list(scratch),
        input_output_aliases=aliases or {},
        compiler_params=pltpu.CompilerParams(vmem_limit_bytes=mib * 1024 * 1024),
        cost_estimate=pl.CostEstimate(flops=flops, bytes_accessed=moved, transcendentals=0),
    )(*args)


def dot(a, b):
    return jnp.dot(a, b, preferred_element_type=jnp.float32)


def dot_nt(a, b):
    return lax.dot_general(a, b, (((1,), (1,)), ((), ())), preferred_element_type=jnp.float32)


def way(self_ref):
    return 1 - 2 * (self_ref[0] & 1)


def earlier_matrix(n, block):
    row = lax.broadcasted_iota(jnp.int32, (n, n), 0)
    col = lax.broadcasted_iota(jnp.int32, (n, n), 1)
    same = (row // block) == (col // block)
    return jnp.where((row < col) & same, 1.0, 0.0).astype(jnp.bfloat16)


def pack_body(self_ref, x_ref, ids_ref, probs_ref, out_ref):
    t = self_ref[1]
    toks = x_ref.shape[0]
    for c in range(8):
        start = pl.multiple_of((c // 2) * 1024 + t * 256 + (c % 2) * 128, 128)
        out_ref[c * toks : (c + 1) * toks, :] = x_ref[:, pl.ds(start, 128)]
    both = jnp.concatenate(
        [ids_ref[...].astype(jnp.float32), probs_ref[...].astype(jnp.float32)], axis=1
    )
    out_ref[8 * toks : 8 * toks + 8, :] = both.astype(jnp.bfloat16)


def prepare_body(w_ref, gate_ref, up_ref, _, out_ref):
    for e in range(2):
        gate = gate_ref[e].astype(jnp.float32)
        hidden = (gate * jax.nn.sigmoid(gate) * up_ref[e].astype(jnp.float32)).astype(jnp.bfloat16)
        for t in range(4):
            for r in range(4):
                start = r * 1024 + t * 256
                out_ref[t, e, :, r * 256 : (r + 1) * 256] = w_ref[e, :, start : start + 256]
            out_ref[t, e, :, 1024:1408] = hidden


def select(self_ref, onehot_ref, code_ref, exp_ref, routes, columns, first):
    s, tokens = self_ref[0], 64 * len(routes)
    routes = [r.astype(jnp.float32) for r in routes]
    ids = jnp.concatenate([r[:, :64] for r in routes], axis=1)
    probs = jnp.concatenate([r[:, 64:] for r in routes], axis=1)
    mine = (2 * (s + way(self_ref) * exp_ref[:, :1]) + exp_ref[:, 1:2]) & 127
    mine = mine.astype(jnp.float32)
    match = jnp.zeros((16, tokens), jnp.float32)
    prob = jnp.zeros((16, tokens), jnp.float32)
    for k in range(8):
        hit = ids[k : k + 1, :] == mine
        match = jnp.where(hit, 1.0, match)
        prob = jnp.where(hit, probs[k : k + 1, :], prob)
    low = match.astype(jnp.bfloat16)
    before = earlier_matrix(min(tokens, 128), 64)
    parts = []
    for c in range(0, tokens, 128):
        part = low[:, c : c + 128]
        parts.append(dot(part, before[: part.shape[1], : part.shape[1]]))
    pos = parts[0] if len(parts) == 1 else jnp.concatenate(parts, axis=1)
    block = (lax.broadcasted_iota(jnp.int32, (16, tokens), 1) >> 6) + first
    code = jnp.where(match > 0.0, pos + 6.0 * block.astype(jnp.float32), -1.0)
    onehot = onehot_ref[...]
    chosen = dot(onehot, code.astype(jnp.bfloat16)) == code_ref[...]
    pick = jnp.where(chosen, 1.0, 0.0).astype(jnp.bfloat16)
    weights = dot(onehot, prob.astype(jnp.bfloat16))
    weighted = jnp.where(chosen, weights, 0.0).astype(jnp.bfloat16)
    slot_probs = dot_nt(jnp.ones((8, tokens), jnp.bfloat16), weighted)
    return [dot(pick, columns(c)) for c in range(8)], slot_probs


def store_pieces(outs, rows, slot_probs, base):
    for c in range(8):
        for v in range(8):
            for e in range(2):
                at = slice(c * 96 + e * 48, c * 96 + (e + 1) * 48)
                part = rows[c][e * 384 + v * 48 : e * 384 + (v + 1) * 48, :].astype(jnp.bfloat16)
                outs[v][at, :] = part if base is None else base[v][at, :] + part
    for v in range(8):
        for c in range(6):
            at = slice(768 + 8 * c, 776 + 8 * c)
            part = slot_probs[:, 128 * c : 128 * (c + 1)].astype(jnp.bfloat16)
            outs[v][at, :] = part if base is None else base[v][at, :] + part


def near_body(self_ref, onehot_ref, code_ref, exp_ref, *refs):
    blocks, outs = refs[:7], refs[7:]

    def columns(c):
        return jnp.concatenate([b[c * 64 : (c + 1) * 64, :] for b in blocks], axis=0)

    routes = [b[512:520, :] for b in blocks]
    rows, probs = select(self_ref, onehot_ref, code_ref, exp_ref, routes, columns, 0)
    store_pieces(outs, rows, probs, None)


def far_body(self_ref, onehot_ref, code_ref, exp_ref, *refs):
    halves, base, outs = refs[:2], refs[2:10], refs[10:]

    def columns(c):
        return halves[c // 4][(c % 4) * 64 : (c % 4 + 1) * 64, :]

    routes = [halves[1][256:264, :]]
    rows, probs = select(self_ref, onehot_ref, code_ref, exp_ref, routes, columns, 7)
    store_pieces(outs, rows, probs, base)


def expert_body(self_ref, place_ref, *refs):
    pieces = refs[:8]
    wh_ref = refs[8]
    gh_refs, gw_refs = refs[9:13], refs[13:17]
    dots_ref, prob_ref = refs[17:19]
    arrived_ref, rows_ref, scaled_ref = refs[19:]
    s, t, r = self_ref[0], self_ref[1], self_ref[2]
    turn = way(self_ref)
    for v in range(8):
        for c in range(8):
            for e in range(2):
                arrived_ref[
                    e * 384 + v * 48 : e * 384 + (v + 1) * 48, c * 128 : (c + 1) * 128
                ] = pieces[v][c * 96 + e * 48 : c * 96 + (e + 1) * 48, :]
    lane = lax.broadcasted_iota(jnp.int32, (8, 768), 1)
    probs = jnp.zeros((8, 768), jnp.float32)
    for v in range(8):
        wide = jnp.concatenate(
            [pieces[v][768 + 8 * c : 776 + 8 * c, :] for c in range(6)], axis=1
        ).astype(jnp.float32)
        mine = place_ref[2:3, :] == v
        probs = jnp.where(mine, wide, probs)
    low = probs.astype(jnp.bfloat16)
    sign = 1 - 2 * ((s + place_ref[3:4, :]) & 1)
    target = ((s + sign * place_ref[0:1, :]) & 63) * 6 + place_ref[1:2, :]
    row = lax.broadcasted_iota(jnp.int32, (384, 384), 0)
    for e in range(2):
        perm = jnp.where(row == target[:, e * 384 : (e + 1) * 384], 1.0, 0.0).astype(jnp.bfloat16)
        mine = low[:, e * 384 : (e + 1) * 384]
        prob_ref[:, e * 384 : (e + 1) * 384] = dot_nt(mine, perm)
        column = dot_nt(perm, mine)[:, :1]
        here = slice(e * 384, (e + 1) * 384)
        for c in range(4):
            part = dot(perm, arrived_ref[here, c * 256 : (c + 1) * 256])
            rows_ref[here, c * 256 : (c + 1) * 256] = part.astype(jnp.bfloat16)
            scaled_ref[here, c * 256 : (c + 1) * 256] = (part * column).astype(jnp.bfloat16)
    for e in range(2):
        total = jnp.zeros((1, 384), jnp.float32)
        for delta in range(4):
            k = (t + turn * delta) & 3
            part = dot_nt(wh_ref[k, e, :, :1024], rows_ref[e * 384 : (e + 1) * 384, :])
            gh_refs[delta][e] = part.astype(jnp.bfloat16)
            hidden = wh_ref[k, e, :, 1024:1408].astype(jnp.float32)
            total += jnp.sum(part * hidden, axis=0, keepdims=True)
        dots_ref[e : e + 1, :] = total
    for e in range(2):
        hidden = jnp.concatenate([wh_ref[k, e, :, 1024:1408] for k in range(4)], axis=0)
        for rho in range(4):
            start = pl.multiple_of(((r + turn * rho) & 3) * 256, 256)
            part = dot(hidden, scaled_ref[e * 384 : (e + 1) * 384, pl.ds(start, 256)])
            part = part.astype(jnp.bfloat16)
            for k in range(4):
                gw_refs[rho][k, e] = part[k * 192 : (k + 1) * 192, :]


def local_body(prob_ref, *refs):
    gh_refs, gate_ref, up_ref, gg_ref, gu_ref = refs[:4], *refs[4:]
    for e in range(2):
        total = gh_refs[0][e].astype(jnp.float32)
        for k in range(1, 4):
            total += gh_refs[k][e].astype(jnp.float32)
        gate = gate_ref[e].astype(jnp.float32)
        up = up_ref[e].astype(jnp.float32)
        sig = jax.nn.sigmoid(gate)
        scaled = prob_ref[0:1, e * 384 : (e + 1) * 384] * total
        gu_ref[e] = (scaled * (gate * sig)).astype(jnp.bfloat16)
        gg_ref[e] = (scaled * up * sig * (1.0 + gate * (1.0 - sig))).astype(jnp.bfloat16)


def replica_body(self_ref, *refs):
    parts, outs = refs[:4], refs[4:]
    for delta in range(4):
        k = (self_ref[1] + way(self_ref) * delta) & 3
        for e in range(2):
            total = parts[0][k, e].astype(jnp.float32)
            for part in parts[1:]:
                total += part[k, e].astype(jnp.float32)
            outs[delta][e] = total.astype(jnp.bfloat16)


def place_body(self_ref, *refs):
    parts, out_ref = refs[:4], refs[4]
    for delta in range(4):
        start = pl.multiple_of(((self_ref[1] - way(self_ref) * delta) & 3) * 256, 256)
        for e in range(2):
            out_ref[e, :, pl.ds(start, 256)] = parts[delta][e]


def lookup_body(ids_ref, table_ref, out_ref):
    experts, capacity = 128, 6
    ids = ids_ref[...]
    expert = lax.broadcasted_iota(jnp.int32, (experts, 64), 0)
    match = jnp.zeros((experts, 64), jnp.float32)
    for k in range(8):
        match = jnp.where(ids[k : k + 1, :] == expert, 1.0, match)
    pos = dot(match.astype(jnp.bfloat16), earlier_matrix(64, 64))
    value = jnp.zeros((experts, 64), jnp.float32)
    for j in range(capacity):
        value = jnp.where(pos == float(j), table_ref[:, j : j + 1], value)
    for k in range(8):
        hit = ids[k : k + 1, :] == expert
        out_ref[k : k + 1, :] = jnp.sum(jnp.where(hit, value, 0.0), axis=0, keepdims=True)


def shifted(x, by, axis):
    count, others = lax.axis_size(axis), lax.axis_size("expert")
    if axis == "expert":
        axes, pairs = axis, [(i, (i + by * (1 - 2 * (i & 1))) % count) for i in range(count)]
    else:
        major = axis == "tensor"
        axes = (axis, "expert") if major else ("expert", axis)

        def at(s, i):
            return i * others + s if major else s * count + i

        pairs = [
            (at(s, i), at(s, (i + by * (1 - 2 * (s & 1))) % count))
            for s in range(others)
            for i in range(count)
        ]
    return lax.ppermute(x, axes, pairs)


def spread(parts, axis):
    return [parts[0], *(shifted(parts[d], d, axis) for d in (1, 2, 3))]


def slot_tables():
    row = np.arange(768)
    onehot = np.zeros((768, 16), np.float32)
    onehot[row, row // 48] = 1.0
    code = (row % 48).astype(np.float32)[:, None]
    shift = np.array(SHIFTS)
    expert = np.stack([np.tile(shift, 2), np.repeat(np.arange(2), 8)], axis=1).astype(np.int32)
    piece, o, j = (row % 384) // 48, (row // 6) % 8, row % 6
    tables = np.zeros((8, 768), np.int32)
    tables[0] = STRIDE * np.array(OFFSETS)[o] - shift[piece]
    tables[1] = j
    tables[2] = piece
    tables[3] = shift[piece] & 1
    return onehot, code, expert, tables


def backward(x, ids, probs, gate, up, w):
    bf16, f32, shape = jnp.bfloat16, jnp.float32, jax.ShapeDtypeStruct
    count = lax.axis_size("expert")
    own = jnp.stack([lax.axis_index(a).astype(jnp.int32) for a in ("expert", "tensor", "dp")])
    ids_t = ids.T
    gate_t = jnp.transpose(gate[0], (0, 2, 1))
    up_t = jnp.transpose(up[0], (0, 2, 1))

    packed = call(pack_body, shape((520, 128), bf16), own, x, ids_t, probs.T, mib=60)
    blocks = {0: packed}
    for step in (1, 2, 3):
        blocks[-step] = shifted(blocks[1 - step], STRIDE, "expert")
        blocks[step] = shifted(blocks[step - 1], -STRIDE, "expert")
    far_low = shifted(blocks[-3][:256], STRIDE, "expert")
    far_high = shifted(blocks[3][256:], -STRIDE, "expert")

    to_send = call(
        prepare_body,
        shape((4, 2, 192, 1408), bf16),
        w,
        gate_t,
        up_t,
        packed,
        untouched=(3,),
        flops=10**7,
        moved=8 * 1024 * 1024, mib=60)
    wh_all = lax.all_to_all(to_send, "tensor", split_axis=0, concat_axis=0, tiled=True)

    onehot, code, expert, tables = slot_tables()
    chooser = (own, jnp.asarray(onehot, bf16), jnp.asarray(code), jnp.asarray(expert))
    near = call(
        near_body,
        [shape((816, 128), bf16)] * 8,
        *chooser,
        *[blocks[o] for o in OFFSETS[:7]],
        flops=10**9,
        moved=4 * 1024 * 1024,
        mib=14,
    )
    pieces = call(
        far_body,
        [shape((816, 128), bf16)] * 8,
        *chooser,
        far_low,
        far_high,
        *near,
        aliases={6 + v: v for v in range(8)},
        flops=10**8,
        moved=4 * 1024 * 1024,
        mib=14,
    )
    pieces = [p if j == 0 else shifted(p, j, "expert") for p, j in zip(pieces, SHIFTS)]

    results = call(
        expert_body,
        [shape((2, 192, 384), bf16)] * 4
        + [shape((4, 2, 192, 256), bf16)] * 4
        + [shape((2, 384), f32), shape((8, 768), f32)],
        own,
        jnp.asarray(tables),
        *pieces,
        wh_all,
        scratch=[
            *[VMEM((768, 1024), bf16)] * 3,
        ],
        flops=6 * 10**9,
        moved=12 * 1024 * 1024, mib=60)
    gh, gw, dots, prob = results[:4], results[4:8], results[8], results[9]

    gw = spread(gw, "dp")
    gh = spread(gh, "tensor")
    cells = jnp.transpose(dots.reshape(2, count, 6), (1, 0, 2)).reshape(count, 12)
    cells = jnp.broadcast_to(cells[None], (4, count, 12)).reshape(4 * count, 12)
    back = lax.all_to_all(cells, ("tensor", "expert"), split_axis=0, concat_axis=0, tiled=True)
    table = back.reshape(4, 2 * count, 6).sum(axis=0)

    summed = call(replica_body, [shape((2, 192, 256), bf16)] * 4, own, *gw, moved=4 * 1024 * 1024, flops=10**7, mib=12)
    summed = spread(summed, "tensor")
    grad_gate, grad_up = call(
        local_body,
        [shape((2, 192, 384), bf16)] * 2,
        prob,
        *gh,
        gate_t,
        up_t,
        flops=10**7,
        moved=4 * 1024 * 1024, mib=10)
    grad_w = call(place_body, shape((2, 192, 1024), bf16), own, *summed, moved=2 * 1024 * 1024, flops=10**6, mib=6)
    grad_probs = call(lookup_body, shape((8, 64), f32), ids_t, table, flops=10**6, moved=10**5, mib=2).T
    return (
        jnp.transpose(grad_gate, (0, 2, 1))[None],
        jnp.transpose(grad_up, (0, 2, 1))[None],
        grad_w,
        grad_probs,
    )


def solution(mesh):
    act = P("dp", "expert", None, "tensor")
    tok = P(("expert", "dp"), None)
    return jax.shard_map(
        backward,
        mesh=mesh,
        in_specs=(tok, tok, tok, act, act, P("expert", "tensor", None)),
        out_specs=(act, act, P("expert", "tensor", "dp"), tok),
        check_vma=False,
    )
```
